32 devices in a mesh: grp: 2 (over x), col: 8 (over z, core), lay: 2 (over y).
Axes of the slice: x: 2, y: 2, z: 4, core: 2. Of those that a mesh axis runs over, the one named last changes fastest.
Arguments:
- gradient: float32 [2, 2, 24, 6144, 128], P('grp', 'lay', None, 'col'), may hold values from -410 to 410
- momentum: float32 [2, 2, 24, 6144, 128], P('grp', 'lay', None, 'col'), may hold values from -820 to 820
- probe_vector: float32 [128], replicated, may hold values from -4 to 4
Outputs:
- new_momentum: float32 [2, 2, 24, 6144, 128], P('grp', 'lay', None, 'col')
- update: float32 [2, 2, 24, 6144, 128], P('grp', 'lay', None, 'col')
The draws below stay inside these ranges and needn't reach their ends.
All inputs are finite; a program needn't handle non-finite values.
Results may differ from the reference program's by a relative error of at most 0.00022.
Values sent between devices are 32-bit elements; how exact they have to be, the bound alone decides.
A program may use at most 128 MiB of HBM per device.

```python
import math
import jax
import jax.numpy as jnp
from jax import lax

D = 6144
HEAD_SIZE = 128
HEADS = 24
ITERS = 3
GROUPS = 2
LAYERS = 2


def shared_scale(key):
    base_key = jax.random.fold_in(key, 7)
    count = GROUPS * LAYERS
    position = jnp.arange(count, dtype=jnp.float32) / max(count - 1, 1)
    rising = jnp.exp(position * jnp.log(3.0))
    row_low, row_high = (0.5, 2.0)
    jitter = jnp.exp(jax.random.uniform(jax.random.fold_in(base_key, 1), (count, HEADS), jnp.float32, jnp.log(0.5), jnp.log(2.0)))
    per_block = (rising[:, None] * jitter).reshape((GROUPS, LAYERS, HEADS, 1, 1))
    row_scale = jnp.exp(jax.random.uniform(jax.random.fold_in(base_key, 2), (GROUPS, LAYERS, HEADS, 1, HEAD_SIZE), jnp.float32, jnp.log(row_low), jnp.log(row_high)))
    return per_block * row_scale


def noise_field(key, salt):
    shape = (GROUPS, LAYERS, HEADS, D, HEAD_SIZE)
    noise = jax.random.truncated_normal(jax.random.fold_in(key, salt), -4.0, 4.0, shape, jnp.float32)
    return noise


def draw_gradient(key, part):
    return (noise_field(key, 11) * shared_scale(key)).astype(jnp.float32)


def draw_momentum(key, part):
    return (2.0 * noise_field(key, 21) * shared_scale(key)).astype(jnp.float32)


def scatter_about(stream_key, dims, scale, limit, held_as=jnp.bfloat16):
    entries = jax.random.normal(stream_key, dims, jnp.float32) * scale
    return jnp.minimum(jnp.maximum(entries, -limit), limit).astype(held_as)


def setup_inputs(seed: int = 0) -> dict:
    arg_keys = jax.random.split(jax.random.key(seed), 4)
    return {
        "gradient": draw_gradient(jax.random.fold_in(arg_keys[3], 71), 0),
        "momentum": draw_momentum(jax.random.fold_in(arg_keys[3], 71), 0),
        "probe_vector": scatter_about(arg_keys[2], (HEAD_SIZE,), 1.0, 4.0, jnp.float32),
    }


MOMENTUM_DECAY = 0.95
LINEAR_TERM = 3.4445
CUBIC_TERM = -4.775
QUINTIC_TERM = 2.0315
EPSILON = 1e-06
PRECISE = lax.Precision.HIGHEST

def reference(gradient, momentum, probe_vector):
    new_momentum = MOMENTUM_DECAY * momentum + gradient
    blend = gradient + MOMENTUM_DECAY * new_momentum
    probe_norm = jnp.sqrt(jnp.sum(probe_vector * probe_vector) + EPSILON)

    def estimate_one(matrix):
        gram_matrix = jnp.dot(matrix.T, matrix, preferred_element_type=jnp.float32, precision=PRECISE)
        product = jnp.dot(gram_matrix, probe_vector, preferred_element_type=jnp.float32, precision=PRECISE)
        return jnp.sqrt(jnp.sum(product * product) + EPSILON) / probe_norm
    stacked = blend.reshape((-1, D, HEAD_SIZE))
    estimate = lax.map(estimate_one, stacked).reshape((GROUPS, LAYERS, HEADS))
    bound_value = 2.0 * jnp.sqrt(lax.optimization_barrier(jnp.max(estimate, axis=(0, 1))))
    scaled = blend / bound_value[None, None, :, None, None]

    def polish(matrix):
        identity = jnp.eye(HEAD_SIZE, dtype=matrix.dtype)
        for counter in range(ITERS):
            gram_matrix = jnp.dot(matrix.T, matrix, preferred_element_type=jnp.float32, precision=PRECISE)
            square = jnp.dot(gram_matrix, gram_matrix, preferred_element_type=jnp.float32, precision=PRECISE)
            mixing = LINEAR_TERM * identity + CUBIC_TERM * gram_matrix + QUINTIC_TERM * square
            matrix = jnp.dot(matrix, mixing, preferred_element_type=jnp.float32, precision=PRECISE)
        return matrix
    polished = lax.map(polish, scaled.reshape((-1, D, HEAD_SIZE))).reshape(blend.shape)
    update = polished * (0.2 * math.sqrt(D))
    return (new_momentum, update)
```

```python
import functools
import math

import jax
import jax.numpy as jnp
from jax import lax
from jax.experimental import pallas as pl
from jax.experimental.pallas import tpu as pltpu
from jax.sharding import PartitionSpec as P

D = 6144
ITERS = 3


MOMENTUM_DECAY = 0.95
LINEAR_TERM = 3.4445
CUBIC_TERM = -4.775
QUINTIC_TERM = 2.0315
EPSILON = 1e-06
PRECISE = lax.Precision.HIGHEST
MESH = pl.DeviceIdType.MESH
CORES = 2
PAD = 8


def split(x):
    high = x.astype(jnp.bfloat16)
    low = (x - high.astype(jnp.float32)).astype(jnp.bfloat16)
    return high, low


def weights(w):
    high, low = split(w)
    top = jnp.concatenate([high, low], axis=1)
    bottom = jnp.concatenate([high, jnp.zeros_like(high)], axis=1)
    return jnp.concatenate([top, bottom], axis=0)


def matmul(x, w_cat):
    n = x.shape[1]
    both = jnp.concatenate(split(x), axis=1)
    out = jnp.dot(both, w_cat, preferred_element_type=jnp.float32)
    return out[:, :n] + out[:, n:]


def places(half, width):
    row = lax.broadcasted_iota(jnp.int32, (half, width), 0)
    lane = lax.broadcasted_iota(jnp.int32, (half, width), 1)
    return row, lane


def pack(sym):
    width = sym.shape[0]
    half = width // 2
    row, lane = places(half, width)
    top, bottom = sym[:half], sym[half:]
    body = jnp.where(lane >= row, top, pltpu.roll(bottom, half, 1))
    diagonal = jnp.sum(jnp.where(lane == row + half, bottom, 0.0), axis=0, keepdims=True)
    return body, jnp.broadcast_to(diagonal, (PAD, width))


def unpack(body, diagonal):
    half, width = body.shape
    row, lane = places(half, width)
    top = jnp.where(lane > row, body, jnp.where(lane == row, 0.5 * body, 0.0))
    rolled = pltpu.roll(body, half, 1)
    bottom = jnp.where((lane >= half) & (lane < row + half), rolled, 0.0)
    bottom = bottom + jnp.where(lane == row + half, 0.5 * diagonal, 0.0)
    tri = jnp.concatenate([top, bottom], axis=0)
    return tri + tri.T


def gram_kernel(gradient, momentum, new_momentum, blend, gram):
    heads, rows, width = blend.shape
    half = width // 2

    def body(g_ref, m_ref, n_ref):
        h = pl.program_id(0)
        g = g_ref[0]
        fresh = MOMENTUM_DECAY * m_ref[0] + g
        n_ref[0] = fresh
        y = g + MOMENTUM_DECAY * fresh
        blend[h] = y
        high, low = split(y)
        both = jnp.concatenate([high, low], axis=1)
        out = lax.dot_general(
            high, both, (((0,), (0,)), ((), ())), preferred_element_type=jnp.float32
        )
        cross = out[:, width:]
        packed, diagonal = pack(out[:, :width] + cross + cross.T)
        gram[h, :half] = packed
        gram[h, half:] = diagonal

    block = pl.BlockSpec((1, rows, width), lambda h: (h, 0, 0))
    pltpu.emit_pipeline(body, grid=(heads,), in_specs=[block, block], out_specs=[block])(
        gradient, momentum, new_momentum
    )


def polish_kernel(sizes, scale, gram, probe, total, sib, acc, up_in, down_in, mine,
                  est_out, est_in, got,
                  sib_send, sib_recv, up_sems, down_sems, est_send, est_recv,
                  out_up, out_down, pair_send, pair_recv):
    n_grp, n_col, n_lay = sizes
    ring = n_col // CORES
    per = gram.shape[1]
    width = gram.shape[3]
    half = width // 2
    up, down = ring // 2, (ring - 1) // 2
    grp, col, lay = lax.axis_index("grp"), lax.axis_index("col"), lax.axis_index("lay")
    z, core = col // CORES, lax.rem(col, CORES)
    way = 1 - 2 * core

    def chip(offset):
        return lax.rem(z + offset + CORES * ring, ring)

    def at(offset, c=core):
        return chip(offset) * CORES + c

    other = 1 - core
    partner = at(0, other)
    ahead, behind = at(way), at(-way)
    peer_count = n_grp * n_lay
    me = grp * n_lay + lay

    def peer(t):
        index = lax.rem(me + t, peer_count)
        return {"grp": index // n_lay, "lay": lax.rem(index, n_lay)}

    neighbours = [{"col": partner}]
    if ring > 1:
        neighbours.append({"col": ahead})
    if ring > 2:
        neighbours.append({"col": behind})
    neighbours += [peer(t) for t in range(1, peer_count)]
    barrier = pltpu.get_barrier_semaphore()
    for neighbour in neighbours:
        pl.semaphore_signal(barrier, inc=1, device_id=neighbour, device_id_type=MESH)
    pl.semaphore_wait(barrier, len(neighbours))

    def send(src, dst, s_sem, r_sem, device):
        return pltpu.make_async_remote_copy(
            src_ref=src, dst_ref=dst, send_sem=s_sem, recv_sem=r_sem,
            device_id=device, device_id_type=MESH,
        )

    offsets = []
    for s in range(max(up, down)):
        if s < up:
            offsets.append(up - s)
        if s < down:
            offsets.append(-(down - s))
    offsets.append(0)
    slot = {o: j for j, o in enumerate(offsets)}

    pair = []
    for j, o in enumerate(offsets):
        copy = send(gram.at[at(-way * o, other)], sib.at[j], sib_send.at[j], sib_recv.at[j],
                    {"col": partner})
        copy.start()
        pair.append(copy)

    def join(o):
        j = slot[o]
        pair[j].wait_recv()
        return gram[at(way * o)] + sib[j]

    flights = []
    flows = []
    for steps, sign, inbox, sems, target in (
        (up, 1, up_in, up_sems, ahead), (down, -1, down_in, down_sems, behind)
    ):
        flows.append((steps, sign, inbox, sems, target, []))
    for s in range(max(up, down)):
        for steps, sign, inbox, sems, target, copies in flows:
            if s >= steps:
                continue
            o = sign * (steps - s)
            j = slot[o]
            value = join(o)
            if s:
                copies[s - 1].wait_recv()
                value = value + inbox[s - 1]
            acc[j] = value
            copy = send(acc.at[j], inbox.at[s], sems.at[0, s], sems.at[1, s], {"col": target})
            copy.start()
            copies.append(copy)
            flights.append(copy)
    value = join(0)
    for steps, sign, inbox, sems, target, copies in flows:
        if steps:
            copies[steps - 1].wait_recv()
            value = value + inbox[steps - 1]
    mine[...] = value

    probe_row = probe[0:1, :]
    probe_norm = jnp.sqrt(jnp.sum(probe_row * probe_row, keepdims=True) + EPSILON)
    grams = []
    for i in range(per):
        full = unpack(mine[i, :half], mine[i, half:half + 1])
        grams.append(full)
        product = jnp.sum(full * probe_row, axis=1, keepdims=True)
        estimate = jnp.sqrt(jnp.sum(product * product, keepdims=True) + EPSILON) / probe_norm
        est_out[i] = jnp.broadcast_to(estimate, (PAD, width))
    shares = []
    for t in range(1, peer_count):
        copy = send(est_out, est_in.at[t - 1], est_send.at[t - 1], est_recv.at[t - 1], peer(t))
        copy.start()
        shares.append(copy)
    for copy in shares:
        copy.wait_recv()
    row, lane = places(width, width)
    identity = jnp.where(row == lane, 1.0, 0.0)
    currents, totals, bounds = [], [], []
    for i in range(per):
        most = est_out[i, 0:1]
        for t in range(1, peer_count):
            most = jnp.maximum(most, est_in[t - 1, i, 0:1])
        bound = 2.0 * jnp.sqrt(most)
        bounds.append(bound)
        currents.append(grams[i] / (bound * bound))
        totals.append(None)
    for counter in range(ITERS):
        cats = [weights(c) for c in currents]
        squares = [matmul(c, w) for c, w in zip(currents, cats)]
        mixing = [
            LINEAR_TERM * identity + CUBIC_TERM * c + QUINTIC_TERM * s
            for c, s in zip(currents, squares)
        ]
        mixed = [weights(m) for m in mixing]
        if counter + 1 < ITERS:
            halfway = [matmul(m, w) for m, w in zip(mixing, cats)]
        totals = [m if t is None else matmul(t, w) for t, m, w in zip(totals, mixing, mixed)]
        if counter + 1 < ITERS:
            currents = [matmul(h, w) for h, w in zip(halfway, mixed)]
    for i in range(per):
        body, diagonal = pack(totals[i] * (scale / bounds[i]))
        got[col, i, :half] = body
        got[col, i, half:] = diagonal

    def spread(index, position):
        copy = send(got.at[index], got.at[index], pair_send.at[position],
                    pair_recv.at[position], {"col": partner})
        copy.start()
        flights.append(copy)

    def pass_on(s, sign, sems, target):
        index = at(-way * sign * s)
        copy = send(got.at[index], got.at[index], sems.at[0, s], sems.at[1, s], {"col": target})
        copy.start()
        flights.append(copy)

    def arrived(index, s_sem, r_sem):
        send(got.at[index], got.at[index], s_sem, r_sem, {"col": partner}).wait_recv()

    def unfold(index):
        for i in range(per):
            total[index * per + i] = unpack(got[index, i, :half], got[index, i, half:half + 1])

    if up:
        pass_on(0, 1, out_up, ahead)
    if down:
        pass_on(0, -1, out_down, behind)
    spread(col, 0)
    unfold(col)
    order = [0]
    for s in range(max(up, down)):
        for steps, sign, sems, target in ((up, 1, out_up, ahead), (down, -1, out_down, behind)):
            if s >= steps:
                continue
            o = -sign * (s + 1)
            index = at(way * o)
            arrived(index, sems.at[0, s], sems.at[1, s])
            if s + 1 < steps:
                pass_on(s + 1, sign, sems, target)
            spread(index, len(order))
            order.append(o)
            unfold(index)
    for position, o in enumerate(order):
        index = at(-way * o, other)
        arrived(index, pair_send.at[position], pair_recv.at[position])
        unfold(index)
    for copy in pair + flights + shares:
        copy.wait_send()


def apply_kernel(blend, total, update):
    heads, rows, width = blend.shape

    def body(u_ref):
        h = pl.program_id(0)
        u_ref[0] = matmul(blend[h], weights(total[h]))

    block = pl.BlockSpec((1, rows, width), lambda h: (h, 0, 0))
    pltpu.emit_pipeline(body, grid=(heads,), in_specs=[], out_specs=[block])(update)


def on_device_kernels(sizes, gradient, momentum, probe_vector):
    n_grp, n_col, n_lay = sizes
    _, _, heads, rows, width = gradient.shape
    per, ring = heads // n_col, n_col // CORES
    depth = width // 2 + PAD
    up, down = ring // 2, (ring - 1) // 2
    peers = max(n_grp * n_lay - 1, 1)
    f32 = jnp.float32
    any_spec, vmem_spec = pl.BlockSpec(memory_space=pl.ANY), pl.BlockSpec(memory_space=pltpu.VMEM)
    limit = 24 * 1024 * 1024
    new_momentum, blend, gram = pl.pallas_call(
        gram_kernel,
        out_shape=(
            jax.ShapeDtypeStruct((heads, rows, width), f32),
            pltpu.VMEM((heads, rows, width), f32),
            pltpu.VMEM((heads, depth, width), f32),
        ),
        in_specs=[any_spec, any_spec],
        out_specs=(any_spec, vmem_spec, vmem_spec),
        compiler_params=pltpu.CompilerParams(vmem_limit_bytes=limit),
        name="gram",
    )(gradient.reshape(heads, rows, width), momentum.reshape(heads, rows, width))
    chunk = (per, depth, width)
    dma = pltpu.SemaphoreType.DMA
    total = pl.pallas_call(
        functools.partial(polish_kernel, sizes, 0.2 * math.sqrt(rows * n_col)),
        out_shape=pltpu.VMEM((heads, width, width), f32),
        in_specs=[vmem_spec, vmem_spec],
        out_specs=vmem_spec,
        scratch_shapes=[
            pltpu.VMEM((ring,) + chunk, f32),
            pltpu.VMEM((ring,) + chunk, f32),
            pltpu.VMEM((max(up, 1),) + chunk, f32),
            pltpu.VMEM((max(down, 1),) + chunk, f32),
            pltpu.VMEM(chunk, f32),
            pltpu.VMEM((per, PAD, width), f32),
            pltpu.VMEM((peers, per, PAD, width), f32),
            pltpu.VMEM((n_col,) + chunk, f32),
            dma((ring,)), dma((ring,)),
            dma((2, max(up, 1))), dma((2, max(down, 1))),
            dma((peers,)), dma((peers,)),
            dma((2, max(up, 1))), dma((2, max(down, 1))),
            dma((ring,)), dma((ring,)),
        ],
        compiler_params=pltpu.CompilerParams(
            collective_id=0, has_side_effects=True, vmem_limit_bytes=limit
        ),
        name="polish",
    )(gram.reshape((n_col,) + chunk), probe_vector.reshape(1, width))
    update = pl.pallas_call(
        apply_kernel,
        out_shape=jax.ShapeDtypeStruct((heads, rows, width), f32),
        in_specs=[vmem_spec, vmem_spec],
        out_specs=any_spec,
        compiler_params=pltpu.CompilerParams(vmem_limit_bytes=limit),
        name="apply",
    )(blend, total)
    return new_momentum.reshape(gradient.shape), update.reshape(gradient.shape)


def summed_gram(stack):
    partial_gram = jnp.einsum("glhdr,glhds->glhrs", stack, stack, precision=PRECISE)
    return lax.psum(partial_gram, "col")


def head_bound(product, probe_norm):
    estimate = jnp.sqrt(jnp.sum(product * product, axis=-1) + EPSILON) / probe_norm
    local_most = jnp.max(estimate, axis=(0, 1))
    overall = lax.pmax(local_most, ("grp", "lay"))
    return 2.0 * jnp.sqrt(overall)


def on_device(gradient, momentum, probe_vector):
    new_momentum = MOMENTUM_DECAY * momentum + gradient
    blend = gradient + MOMENTUM_DECAY * new_momentum
    width = blend.shape[-1]
    probe_norm = jnp.sqrt(jnp.sum(probe_vector * probe_vector) + EPSILON)
    raw_gram = summed_gram(blend)
    product = jnp.einsum("glhrs,s->glhr", raw_gram, probe_vector, precision=PRECISE)
    bound_value = head_bound(product, probe_norm)
    scaled = blend / bound_value[None, None, :, None, None]
    current = raw_gram / (bound_value * bound_value)[None, None, :, None, None]
    identity = jnp.eye(width, dtype=jnp.float32)
    total = jnp.broadcast_to(identity, current.shape)
    for counter in range(ITERS):
        square = jnp.einsum("glhrs,glhst->glhrt", current, current, precision=PRECISE)
        mixing = LINEAR_TERM * identity + CUBIC_TERM * current + QUINTIC_TERM * square
        total = jnp.einsum("glhrs,glhst->glhrt", total, mixing, precision=PRECISE)
        if counter + 1 < ITERS:
            halfway = jnp.einsum("glhrs,glhst->glhrt", mixing, current, precision=PRECISE)
            current = jnp.einsum("glhrs,glhst->glhrt", halfway, mixing, precision=PRECISE)
    polished = jnp.einsum("glhdr,glhrs->glhds", scaled, total, precision=PRECISE)
    update = polished * (0.2 * math.sqrt(D))
    return (new_momentum, update)


def solution(mesh):
    sizes = (mesh.shape["grp"], mesh.shape["col"], mesh.shape["lay"])

    def local(gradient, momentum, probe_vector):
        heads = gradient.shape[2]
        whole_heads = heads % sizes[1] == 0 and sizes[1] % CORES == 0
        if whole_heads and gradient.shape[:2] == (1, 1):
            return on_device_kernels(sizes, gradient, momentum, probe_vector)
        return on_device(gradient, momentum, probe_vector)

    in_specs = (P("grp", "lay", None, "col", None), P("grp", "lay", None, "col", None), P())
    out_specs = (P("grp", "lay", None, "col", None), P("grp", "lay", None, "col", None))
    return jax.shard_map(
        local, mesh=mesh, in_specs=in_specs, out_specs=out_specs, check_vma=False
    )
```

```python
import functools
import math

import jax
import jax.numpy as jnp
from jax import lax
from jax.experimental import pallas as pl
from jax.experimental.pallas import tpu as pltpu
from jax.sharding import PartitionSpec as P

D = 6144
ITERS = 3


MOMENTUM_DECAY = 0.95
LINEAR_TERM = 3.4445
CUBIC_TERM = -4.775
QUINTIC_TERM = 2.0315
EPSILON = 1e-06
PRECISE = lax.Precision.HIGHEST
MESH = pl.DeviceIdType.MESH
CORES = 2
PAD = 8
BUFFERS = 3


def split(x):
    high = x.astype(jnp.bfloat16)
    low = (x - high.astype(jnp.float32)).astype(jnp.bfloat16)
    return high, low


def weights(w):
    high, low = split(w)
    top = jnp.concatenate([high, low], axis=1)
    bottom = jnp.concatenate([high, jnp.zeros_like(high)], axis=1)
    return jnp.concatenate([top, bottom], axis=0)


def matmul(x, w_cat):
    n = x.shape[1]
    both = jnp.concatenate(split(x), axis=1)
    out = jnp.dot(both, w_cat, preferred_element_type=jnp.float32)
    return out[:, :n] + out[:, n:]


def places(half, width):
    row = lax.broadcasted_iota(jnp.int32, (half, width), 0)
    lane = lax.broadcasted_iota(jnp.int32, (half, width), 1)
    return row, lane


def pack(sym):
    width = sym.shape[0]
    half = width // 2
    row, lane = places(half, width)
    top, bottom = sym[:half], sym[half:]
    body = jnp.where(lane >= row, top, pltpu.roll(bottom, half, 1))
    diagonal = jnp.sum(jnp.where(lane == row + half, bottom, 0.0), axis=0, keepdims=True)
    return body, jnp.broadcast_to(diagonal, (PAD, width))


def unpack(body, diagonal):
    half, width = body.shape
    row, lane = places(half, width)
    top = jnp.where(lane > row, body, jnp.where(lane == row, 0.5 * body, 0.0))
    rolled = pltpu.roll(body, half, 1)
    bottom = jnp.where((lane >= half) & (lane < row + half), rolled, 0.0)
    bottom = bottom + jnp.where(lane == row + half, 0.5 * diagonal, 0.0)
    tri = jnp.concatenate([top, bottom], axis=0)
    return tri + tri.T


def polish_kernel(sizes, scale, gradient, momentum, probe, new_momentum, blend, total,
                  g_in, m_in, gram, sib, acc, up_in, down_in, mine,
                  est_out, est_in, got, g_sem, m_sem,
                  sib_send, sib_recv, up_sems, down_sems, est_send, est_recv,
                  out_up, out_down, pair_send, pair_recv):
    n_grp, n_col, n_lay = sizes
    ring = n_col // CORES
    per = gram.shape[1]
    width = gram.shape[3]
    half = width // 2
    depth = g_in.shape[0]
    up, down = ring // 2, (ring - 1) // 2
    grp, col, lay = lax.axis_index("grp"), lax.axis_index("col"), lax.axis_index("lay")
    z, core = col // CORES, lax.rem(col, CORES)
    way = 1 - 2 * core

    def chip(offset):
        return lax.rem(z + offset + CORES * ring, ring)

    def at(offset, c=core):
        return chip(offset) * CORES + c

    other = 1 - core
    partner = at(0, other)
    ahead, behind = at(way), at(-way)
    peer_count = n_grp * n_lay
    me = grp * n_lay + lay

    def peer(t):
        index = lax.rem(me + t, peer_count)
        return {"grp": index // n_lay, "lay": lax.rem(index, n_lay)}

    neighbours = [{"col": partner}]
    if ring > 1:
        neighbours.append({"col": ahead})
    if ring > 2:
        neighbours.append({"col": behind})
    neighbours += [peer(t) for t in range(1, peer_count)]
    barrier = pltpu.get_barrier_semaphore()
    for neighbour in neighbours:
        pl.semaphore_signal(barrier, inc=1, device_id=neighbour, device_id_type=MESH)

    def send(src, dst, s_sem, r_sem, device):
        return pltpu.make_async_remote_copy(
            src_ref=src, dst_ref=dst, send_sem=s_sem, recv_sem=r_sem,
            device_id=device, device_id_type=MESH,
        )

    offsets = []
    for s in range(max(up, down)):
        if s < up:
            offsets.append(up - s)
        if s < down:
            offsets.append(-(down - s))
    offsets.append(0)
    slot = {o: j for j, o in enumerate(offsets)}

    def offset_of(j):
        return sum(o * jnp.where(j == i, 1, 0) for i, o in enumerate(offsets) if o)

    def owner(t):
        own = lax.rem(t, 2)
        place = chip((2 * own - 1) * way * offset_of(t // 2))
        return place * CORES + lax.rem(core + 1 + own, CORES)

    def loads(t):
        heads = pl.ds(owner(t) * per, per)
        b = lax.rem(t, depth)
        return (
            pltpu.make_async_copy(gradient.at[heads], g_in.at[b], g_sem.at[b]),
            pltpu.make_async_copy(momentum.at[heads], m_in.at[b], m_sem.at[b]),
        )

    def pair_copy(j):
        return send(gram.at[at(-way * offsets[j], other)], sib.at[j],
                    sib_send.at[j], sib_recv.at[j], {"col": partner})

    flows = ((up, 1, up_in, up_sems, ahead), (down, -1, down_in, down_sems, behind))

    def flow_copy(flow, s):
        steps, sign, inbox, sems, target = flow
        return send(acc.at[slot[sign * (steps - s)]], inbox.at[s],
                    sems.at[0, s], sems.at[1, s], {"col": target})

    hops = []
    for s in range(max(up, down)):
        hops += [(flow, s) for flow in flows if s < flow[0]]

    def join(j):
        pair_copy(j).wait_recv()
        value = gram[at(way * offsets[j])] + sib[j]
        if j + 1 == ring:
            for flow in flows:
                if flow[0]:
                    flow_copy(flow, flow[0] - 1).wait_recv()
                    value = value + flow[2][flow[0] - 1]
            mine[...] = value
            return
        flow, s = hops[j]
        if s:
            flow_copy(flow, s - 1).wait_recv()
            value = value + flow[2][s - 1]
        acc[j] = value
        flow_copy(flow, s).start()

    steps = 2 * ring
    for t in range(min(depth - 1, steps)):
        for copy in loads(t):
            copy.start()

    pl.semaphore_wait(barrier, len(neighbours))

    @pl.loop(0, steps)
    def _(t):
        @pl.when(t + depth - 1 < steps)
        def _():
            for copy in loads(t + depth - 1):
                copy.start()

        for copy in loads(t):
            copy.wait()
        index, b = owner(t), lax.rem(t, depth)
        for i in range(per):
            h = index * per + i
            g = g_in[b, i]
            fresh = MOMENTUM_DECAY * m_in[b, i] + g
            new_momentum[h] = fresh
            high, low = split(g + MOMENTUM_DECAY * fresh)
            both = jnp.concatenate([high, low], axis=1)
            blend[h] = both
            out = lax.dot_general(
                high, both, (((0,), (0,)), ((), ())), preferred_element_type=jnp.float32
            )
            cross = out[:, width:]
            packed, diagonal = pack(out[:, :width] + cross + cross.T)
            gram[index, i, :half] = packed
            gram[index, i, half:] = diagonal
        for j in range(ring):
            pl.when(t == 2 * j)(lambda j=j: pair_copy(j).start())
            pl.when(t == 2 * j + 1)(functools.partial(join, j))

    flights = []
    probe_row = probe[0:1, :]
    probe_norm = jnp.sqrt(jnp.sum(probe_row * probe_row, keepdims=True) + EPSILON)
    grams = []
    for i in range(per):
        full = unpack(mine[i, :half], mine[i, half:half + 1])
        grams.append(full)
        product = jnp.sum(full * probe_row, axis=1, keepdims=True)
        estimate = jnp.sqrt(jnp.sum(product * product, keepdims=True) + EPSILON) / probe_norm
        est_out[i] = jnp.broadcast_to(estimate, (PAD, width))
    shares = []
    for t in range(1, peer_count):
        copy = send(est_out, est_in.at[t - 1], est_send.at[t - 1], est_recv.at[t - 1], peer(t))
        copy.start()
        shares.append(copy)
    for copy in shares:
        copy.wait_recv()
    row, lane = places(width, width)
    identity = jnp.where(row == lane, 1.0, 0.0)
    currents, totals, bounds = [], [], []
    for i in range(per):
        most = est_out[i, 0:1]
        for t in range(1, peer_count):
            most = jnp.maximum(most, est_in[t - 1, i, 0:1])
        bound = 2.0 * jnp.sqrt(most)
        bounds.append(bound)
        currents.append(grams[i] / (bound * bound))
        totals.append(None)
    for counter in range(ITERS):
        cats = [weights(c) for c in currents]
        squares = [matmul(c, w) for c, w in zip(currents, cats)]
        mixing = [
            LINEAR_TERM * identity + CUBIC_TERM * c + QUINTIC_TERM * s
            for c, s in zip(currents, squares)
        ]
        mixed = [weights(m) for m in mixing]
        if counter + 1 < ITERS:
            halfway = [matmul(m, w) for m, w in zip(mixing, cats)]
        totals = [m if t is None else matmul(t, w) for t, m, w in zip(totals, mixing, mixed)]
        if counter + 1 < ITERS:
            currents = [matmul(h, w) for h, w in zip(halfway, mixed)]
    for i in range(per):
        body, diagonal = pack(totals[i] * (scale / bounds[i]))
        got[col, i, :half] = body
        got[col, i, half:] = diagonal

    def spread(index, position):
        copy = send(got.at[index], got.at[index], pair_send.at[position],
                    pair_recv.at[position], {"col": partner})
        copy.start()
        flights.append(copy)

    def pass_on(s, sign, sems, target):
        index = at(-way * sign * s)
        copy = send(got.at[index], got.at[index], sems.at[0, s], sems.at[1, s], {"col": target})
        copy.start()
        flights.append(copy)

    def arrived(index, s_sem, r_sem):
        send(got.at[index], got.at[index], s_sem, r_sem, {"col": partner}).wait_recv()

    def unfold(index):
        for i in range(per):
            full = unpack(got[index, i, :half], got[index, i, half:half + 1])
            total[index * per + i] = weights(full)

    if up:
        pass_on(0, 1, out_up, ahead)
    if down:
        pass_on(0, -1, out_down, behind)
    spread(col, 0)
    unfold(col)
    order = [0]
    for s in range(max(up, down)):
        for steps, sign, sems, target in ((up, 1, out_up, ahead), (down, -1, out_down, behind)):
            if s >= steps:
                continue
            o = -sign * (s + 1)
            index = at(way * o)
            arrived(index, sems.at[0, s], sems.at[1, s])
            if s + 1 < steps:
                pass_on(s + 1, sign, sems, target)
            spread(index, len(order))
            order.append(o)
            unfold(index)
    for position, o in enumerate(order):
        index = at(-way * o, other)
        arrived(index, pair_send.at[position], pair_recv.at[position])
        unfold(index)
    for j in range(ring):
        pair_copy(j).wait_send()
    for flow, s in hops:
        flow_copy(flow, s).wait_send()
    for copy in flights + shares:
        copy.wait_send()


def apply_kernel(per, fresh, blend, total, new_momentum, update, sem):
    heads, rows, width = fresh.shape
    copy = pltpu.make_async_copy(fresh, new_momentum, sem)
    copy.start()

    def body(u_ref):
        step = pl.program_id(0)
        for i in range(per):
            h = step * per + i
            out = jnp.dot(blend[h], total[h], preferred_element_type=jnp.float32)
            u_ref[i] = out[:, :width] + out[:, width:]

    block = pl.BlockSpec((per, rows, width), lambda s: (s, 0, 0))
    pltpu.emit_pipeline(body, grid=(heads // per,), in_specs=[], out_specs=[block])(update)
    copy.wait()


def on_device_kernels(sizes, gradient, momentum, probe_vector):
    n_grp, n_col, n_lay = sizes
    _, _, heads, rows, width = gradient.shape
    per, ring = heads // n_col, n_col // CORES
    depth = width // 2 + PAD
    up, down = ring // 2, (ring - 1) // 2
    peers = max(n_grp * n_lay - 1, 1)
    f32, bf16 = jnp.float32, jnp.bfloat16
    any_spec, vmem_spec = pl.BlockSpec(memory_space=pl.ANY), pl.BlockSpec(memory_space=pltpu.VMEM)
    limit = 24 * 1024 * 1024
    chunk = (per, depth, width)
    dma = pltpu.SemaphoreType.DMA
    fresh, blend, total = pl.pallas_call(
        functools.partial(polish_kernel, sizes, 0.2 * math.sqrt(rows * n_col)),
        out_shape=(
            pltpu.VMEM((heads, rows, width), f32),
            pltpu.VMEM((heads, rows, 2 * width), bf16),
            pltpu.VMEM((heads, 2 * width, 2 * width), bf16),
        ),
        in_specs=[any_spec, any_spec, vmem_spec],
        out_specs=(vmem_spec, vmem_spec, vmem_spec),
        scratch_shapes=[
            pltpu.VMEM((BUFFERS, per, rows, width), f32),
            pltpu.VMEM((BUFFERS, per, rows, width), f32),
            pltpu.VMEM((n_col,) + chunk, f32),
            pltpu.VMEM((ring,) + chunk, f32),
            pltpu.VMEM((ring,) + chunk, f32),
            pltpu.VMEM((max(up, 1),) + chunk, f32),
            pltpu.VMEM((max(down, 1),) + chunk, f32),
            pltpu.VMEM(chunk, f32),
            pltpu.VMEM((per, PAD, width), f32),
            pltpu.VMEM((peers, per, PAD, width), f32),
            pltpu.VMEM((n_col,) + chunk, f32),
            dma((BUFFERS,)), dma((BUFFERS,)),
            dma((ring,)), dma((ring,)),
            dma((2, max(up, 1))), dma((2, max(down, 1))),
            dma((peers,)), dma((peers,)),
            dma((2, max(up, 1))), dma((2, max(down, 1))),
            dma((ring,)), dma((ring,)),
        ],
        compiler_params=pltpu.CompilerParams(
            collective_id=0, has_side_effects=True, vmem_limit_bytes=limit
        ),
        name="polish",
    )(
        pltpu.with_memory_space_constraint(gradient.reshape(heads, rows, width), pltpu.HBM),
        pltpu.with_memory_space_constraint(momentum.reshape(heads, rows, width), pltpu.HBM),
        probe_vector.reshape(1, width),
    )
    new_momentum, update = pl.pallas_call(
        functools.partial(apply_kernel, per),
        out_shape=(jax.ShapeDtypeStruct((heads, rows, width), f32),) * 2,
        in_specs=[vmem_spec, vmem_spec, vmem_spec],
        out_specs=(any_spec, any_spec),
        scratch_shapes=[dma],
        compiler_params=pltpu.CompilerParams(vmem_limit_bytes=limit),
        name="apply",
    )(fresh, blend, total)
    return new_momentum.reshape(gradient.shape), update.reshape(gradient.shape)


def summed_gram(stack):
    partial_gram = jnp.einsum("glhdr,glhds->glhrs", stack, stack, precision=PRECISE)
    return lax.psum(partial_gram, "col")


def head_bound(product, probe_norm):
    estimate = jnp.sqrt(jnp.sum(product * product, axis=-1) + EPSILON) / probe_norm
    local_most = jnp.max(estimate, axis=(0, 1))
    overall = lax.pmax(local_most, ("grp", "lay"))
    return 2.0 * jnp.sqrt(overall)


def on_device(gradient, momentum, probe_vector):
    new_momentum = MOMENTUM_DECAY * momentum + gradient
    blend = gradient + MOMENTUM_DECAY * new_momentum
    width = blend.shape[-1]
    probe_norm = jnp.sqrt(jnp.sum(probe_vector * probe_vector) + EPSILON)
    raw_gram = summed_gram(blend)
    product = jnp.einsum("glhrs,s->glhr", raw_gram, probe_vector, precision=PRECISE)
    bound_value = head_bound(product, probe_norm)
    scaled = blend / bound_value[None, None, :, None, None]
    current = raw_gram / (bound_value * bound_value)[None, None, :, None, None]
    identity = jnp.eye(width, dtype=jnp.float32)
    total = jnp.broadcast_to(identity, current.shape)
    for counter in range(ITERS):
        square = jnp.einsum("glhrs,glhst->glhrt", current, current, precision=PRECISE)
        mixing = LINEAR_TERM * identity + CUBIC_TERM * current + QUINTIC_TERM * square
        total = jnp.einsum("glhrs,glhst->glhrt", total, mixing, precision=PRECISE)
        if counter + 1 < ITERS:
            halfway = jnp.einsum("glhrs,glhst->glhrt", mixing, current, precision=PRECISE)
            current = jnp.einsum("glhrs,glhst->glhrt", halfway, mixing, precision=PRECISE)
    polished = jnp.einsum("glhdr,glhrs->glhds", scaled, total, precision=PRECISE)
    update = polished * (0.2 * math.sqrt(D))
    return (new_momentum, update)


def solution(mesh):
    sizes = (mesh.shape["grp"], mesh.shape["col"], mesh.shape["lay"])

    def local(gradient, momentum, probe_vector):
        heads = gradient.shape[2]
        whole_heads = heads % sizes[1] == 0 and sizes[1] % CORES == 0
        if whole_heads and gradient.shape[:2] == (1, 1):
            return on_device_kernels(sizes, gradient, momentum, probe_vector)
        return on_device(gradient, momentum, probe_vector)

    in_specs = (P("grp", "lay", None, "col", None), P("grp", "lay", None, "col", None), P())
    out_specs = (P("grp", "lay", None, "col", None), P("grp", "lay", None, "col", None))
    return jax.shard_map(
        local, mesh=mesh, in_specs=in_specs, out_specs=out_specs, check_vma=False
    )
```
